256 devices in a mesh: rows: 64 (over x_hi, z, y), cols: 4 (over x_lo, core).
Axes of the slice: x: 4 (x_hi: 2, x_lo: 2; x = x_hi * 2 + x_lo), y: 4, z: 8, core: 2. Of those that a mesh axis runs over, the one named last changes fastest.
Arguments:
- tokens: bfloat16 [768, 96, 768], P('rows', 'cols'), may hold values from -48 to 48
- ln_gain: float32 [768], replicated, may hold values from 0.5 to 1.5
- ln_bias: float32 [768], replicated, may hold values from -3 to 3
- qkv_weight: bfloat16 [768, 2304], replicated, may hold values from -3 to 3
- qkv_bias: float32 [2304], replicated, may hold values from -3 to 3
- rel_table: float32 [23, 23, 24], replicated, may hold values from -4 to 4
- proj_weight: bfloat16 [768, 768], replicated, may hold values from -0.21875 to 0.21875
- proj_bias: float32 [768], replicated, may hold values from -3 to 3
- branch_weight: bfloat16 [4, 768, 512], replicated, may hold values from -0.21875 to 0.21875
- branch_bias: float32 [4, 512], replicated, may hold values from -4 to 4
- join_block: bfloat16 [768, 512], replicated, may hold values from -0.109375 to 0.109375
- join_branch: bfloat16 [4, 512, 512], replicated, may hold values from -0.375 to 0.375
- bn_gain: float32 [512], replicated, may hold values from 0.25 to 1.75
- bn_bias: float32 [512], replicated, may hold values from -4 to 4
Outputs:
- joined: bfloat16 [768, 96, 512], P('rows', 'cols')
The draws below stay inside these ranges and needn't reach their ends.
All inputs are finite; a program needn't handle non-finite values.
Results may differ from the reference program's by a relative error of at most 0.0049.
Values may be sent and summed in bfloat16 or wider, within the bound.
A program may use at most 128 MiB of HBM per device.

```python
import math
import jax
import jax.numpy as jnp
from jax import lax

D = 768
HEADS = 24
CH = 512
WIN = 12
HEIGHT = 768
WIDTH = 96


def draw_tokens(key, part):
    subkeys = jax.random.split(jax.random.fold_in(key, 11), 10)
    row_index = jnp.arange(HEIGHT, dtype=jnp.int32)
    row_frac = row_index.astype(jnp.float32)[:, None, None] / HEIGHT
    col_frac = jnp.arange(WIDTH, dtype=jnp.float32)[None, :, None] / WIDTH
    coarse = jax.random.truncated_normal(subkeys[1], -3.0, 3.0, (HEIGHT // 4, WIDTH // 4, D), jnp.float32)
    coarse = jnp.repeat(jnp.repeat(coarse, 4, axis=0), 4, axis=1)
    row_slope = jax.random.truncated_normal(subkeys[2], -3.0, 3.0, (D,), jnp.float32)
    col_tilt = jax.random.truncated_normal(subkeys[3], -3.0, 3.0, (D,), jnp.float32)
    trend_part = row_slope * (1.0 + 2.0 * row_frac) + 0.5 * col_tilt * col_frac
    band_rows = 4 * WIN
    band_count = HEIGHT // band_rows + 1
    band_levels = jnp.exp(jax.random.uniform(subkeys[5], (band_count,), jnp.float32, math.log(1.0 / 3.0), math.log(3.0)))
    band_onehot = (row_index[:, None] // band_rows == jnp.arange(band_count, dtype=jnp.int32)[None, :]).astype(jnp.float32)
    band_factor = jnp.sum(band_onehot * band_levels[None, :], 1)[:, None, None]
    row_amp = jax.random.uniform(subkeys[6], (D,), jnp.float32, 0.5, 1.0)
    col_amp = jax.random.uniform(subkeys[7], (D,), jnp.float32, 0.5, 1.0)
    row_phase = jax.random.uniform(subkeys[8], (D,), jnp.float32, 0.0, 2.0 * math.pi)
    col_phase = jax.random.uniform(subkeys[9], (D,), jnp.float32, 0.0, 2.0 * math.pi)
    smooth_part = 8.0 * row_amp * jnp.cos(6.0 * math.pi * row_frac + row_phase) + 4.0 * col_amp * jnp.cos(6.0 * math.pi * col_frac + col_phase)
    noise_part = jax.random.truncated_normal(subkeys[0], -3.0, 3.0, (HEIGHT, WIDTH, D), jnp.float32)
    values = band_factor * (0.8 * noise_part + 0.6 * coarse) + trend_part + smooth_part
    values = jnp.clip(values, -47.5, 47.5)
    return values.astype(jnp.bfloat16)


def draw_qkv_weight(key, part):
    base = jax.random.truncated_normal(jax.random.fold_in(key, 23), -3.0, 3.0, (D, 3 * D), jnp.float32) / math.sqrt(D)
    return base.astype(jnp.bfloat16)


def bell_draw(stream_key, dims, scale, most, kind=jnp.bfloat16):
    return jnp.clip(scale * jax.random.normal(stream_key, dims, jnp.float32), -most, most).astype(kind)


def setup_inputs(seed: int = 0) -> dict:
    arg_keys = jax.random.split(jax.random.key(seed), 15)
    tokens = draw_tokens(jax.random.fold_in(arg_keys[14], 71), 0)
    ln_gain = jnp.clip(1.0 + 0.1 * jax.random.normal(arg_keys[1], (D,), jnp.float32), 0.5, 1.5)
    ln_bias = bell_draw(arg_keys[2], (D,), 0.5, 3.0, jnp.float32)
    qkv_weight = draw_qkv_weight(jax.random.fold_in(arg_keys[14], 71), 0)
    qkv_bias = bell_draw(arg_keys[4], (3 * D,), 0.5, 3.0, jnp.float32)
    rel_table = bell_draw(arg_keys[5], (2 * WIN - 1, 2 * WIN - 1, HEADS), 1.0, 4.0, jnp.float32)
    proj_weight = bell_draw(arg_keys[6], (D, D), D ** -0.5, 0.21875)
    proj_bias = bell_draw(arg_keys[7], (D,), 0.5, 3.0, jnp.float32)
    branch_weight = bell_draw(arg_keys[8], (4, D, CH), D ** -0.5, 0.21875)
    branch_bias = bell_draw(arg_keys[9], (4, CH), 1.0, 4.0, jnp.float32)
    join_block = bell_draw(arg_keys[10], (D, CH), (D + 4 * CH) ** -0.5, 0.109375)
    join_branch = bell_draw(arg_keys[11], (4, CH, CH), (CH // 2) ** -0.5, 0.375)
    bn_gain = jnp.clip(1.0 + 0.15 * jax.random.normal(arg_keys[12], (CH,), jnp.float32), 0.25, 1.75)
    bn_bias = bell_draw(arg_keys[13], (CH,), 1.0, 4.0, jnp.float32)
    return {"tokens": tokens, "ln_gain": ln_gain, "ln_bias": ln_bias, "qkv_weight": qkv_weight, "qkv_bias": qkv_bias, "rel_table": rel_table, "proj_weight": proj_weight, "proj_bias": proj_bias, "branch_weight": branch_weight, "branch_bias": branch_bias, "join_block": join_block, "join_branch": join_branch, "bn_gain": bn_gain, "bn_bias": bn_bias}


bin_scales = (1, 2, 3, 6)
bin_starts = (0, 1, 3, 6)
norm_eps = 1e-05
highest = lax.Precision.HIGHEST

def layer_norm(values, norm_gain, norm_bias):
    floats = values.astype(jnp.float32)
    center = lax.optimization_barrier(jnp.mean(floats, -1, keepdims=True))
    spread_sq = lax.optimization_barrier(jnp.mean(jnp.square(floats - center), -1, keepdims=True))
    return ((floats - center) * lax.rsqrt(spread_sq + norm_eps) * norm_gain + norm_bias).astype(jnp.bfloat16)

def relative_bias(rel_table):
    steps_idx = jnp.arange(WIN, dtype=jnp.int32)
    offsets = steps_idx[:, None] - steps_idx[None, :] + WIN - 1
    onehot = (offsets[:, :, None] == jnp.arange(2 * WIN - 1, dtype=jnp.int32)[None, None, :]).astype(jnp.float32)
    pair_bias = jnp.einsum('pra,qsb,abh->hpqrs', onehot, onehot, rel_table, precision=highest)
    return pair_bias.reshape(rel_table.shape[2], WIN * WIN, WIN * WIN)

def region_labels(positions, total):
    return (positions >= total - WIN).astype(jnp.int32) + (positions >= total - WIN // 2).astype(jnp.int32)

def window_mask(row_place, col_place, height, breadth):
    labels = 3 * region_labels(row_place, height)[:, None] + region_labels(col_place, breadth)[None, :]
    labels = labels.reshape(row_place.shape[0] // WIN, WIN, col_place.shape[0] // WIN, WIN)
    labels = labels.transpose(0, 2, 1, 3).reshape(-1, WIN * WIN)
    return jnp.where(labels[:, :, None] != labels[:, None, :], -100.0, 0.0).astype(jnp.float32)

def window_attention(normed, qkv_weight, qkv_bias, proj_weight, proj_bias, pair_bias, mask_add):
    row_count, col_count, width = normed.shape
    heads_count = pair_bias.shape[0]
    head_size = width // heads_count
    windows = normed.reshape(row_count // WIN, WIN, col_count // WIN, WIN, width)
    windows = windows.transpose(0, 2, 1, 3, 4).reshape(-1, WIN * WIN, width)
    count_win = windows.shape[0]
    mixed = jnp.dot(windows.reshape(-1, width), qkv_weight, preferred_element_type=jnp.float32) + qkv_bias
    mixed = mixed.reshape(count_win, WIN * WIN, 3, heads_count, head_size)
    queries = (mixed[:, :, 0] * head_size ** (-0.5)).astype(jnp.bfloat16)
    keys_bf = mixed[:, :, 1].astype(jnp.bfloat16)
    values_bf = mixed[:, :, 2].astype(jnp.bfloat16)
    scores = jnp.einsum('wihd,wjhd->whij', queries.astype(jnp.float32), keys_bf.astype(jnp.float32))
    scores = scores + pair_bias[None] + mask_add[:, None]
    weights = jax.nn.softmax(scores, axis=-1).astype(jnp.bfloat16)
    context = jnp.einsum('whij,wjhd->wihd', weights.astype(jnp.float32), values_bf.astype(jnp.float32))
    context = context.astype(jnp.bfloat16).reshape(-1, width)
    output = jnp.dot(context, proj_weight, preferred_element_type=jnp.float32) + proj_bias
    output = output.reshape(row_count // WIN, col_count // WIN, WIN, WIN, width).transpose(0, 2, 1, 3, 4)
    return output.reshape(row_count, col_count, width)

def bin_tables(positions, total):
    pooling = []
    spread = []
    place_f = positions.astype(jnp.float32)
    for scale_value in bin_scales:
        levels = jnp.arange(scale_value, dtype=jnp.int32)
        pooling.append((positions[:, None] // (total // scale_value) == levels[None, :]).astype(jnp.float32))
        source = jnp.clip((place_f + 0.5) * (scale_value / total) - 0.5, 0.0, scale_value - 1.0)
        spread.append(jax.nn.relu(1.0 - jnp.abs(source[:, None] - levels[None, :].astype(jnp.float32))))
    return (jnp.concatenate(pooling, 1), jnp.concatenate(spread, 1))

def branch_projections(pooled, branch_weight, branch_bias, join_branch):
    results = []
    start_row = 0
    for branch_index, scale_value in enumerate(bin_scales):
        cell_rows = pooled[start_row:start_row + scale_value * scale_value]
        hidden_map = jax.nn.relu(jnp.dot(cell_rows, branch_weight[branch_index].astype(jnp.float32), precision=highest) + branch_bias[branch_index])
        results.append(jnp.dot(hidden_map, join_branch[branch_index].astype(jnp.float32), precision=highest))
        start_row += scale_value * scale_value
    return jnp.concatenate(results, 0)

def spread_cells(projected, row_spread, col_spread):
    total_map = jnp.zeros((row_spread.shape[0], col_spread.shape[0], projected.shape[1]), jnp.float32)
    start_row = 0
    for scale_value, start_value in zip(bin_scales, bin_starts):
        block_cells = projected[start_row:start_row + scale_value * scale_value].reshape(scale_value, scale_value, -1)
        across = jnp.einsum('cb,abh->ach', col_spread[:, start_value:start_value + scale_value], block_cells, precision=highest)
        total_map = total_map + jnp.einsum('ra,ach->rch', row_spread[:, start_value:start_value + scale_value], across, precision=highest)
        start_row += scale_value * scale_value
    return total_map

def reference(tokens, ln_gain, ln_bias, qkv_weight, qkv_bias, rel_table, proj_weight, proj_bias, branch_weight, branch_bias, join_block, join_branch, bn_gain, bn_bias):
    half = WIN // 2
    rolled_tok = jnp.roll(tokens, (-half, -half), (0, 1))
    normed = layer_norm(rolled_tok, ln_gain, ln_bias)
    pair_bias = relative_bias(rel_table)
    col_place = jnp.arange(WIDTH, dtype=jnp.int32)

    def one_strip(start_row):
        strip = lax.dynamic_slice_in_dim(normed, start_row, WIN, 0)
        row_place = start_row + jnp.arange(WIN, dtype=jnp.int32)
        mask_add = window_mask(row_place, col_place, HEIGHT, WIDTH)
        return window_attention(strip, qkv_weight, qkv_bias, proj_weight, proj_bias, pair_bias, mask_add)
    starts = (jnp.arange(HEIGHT // WIN, dtype=jnp.int32) * WIN).astype(jnp.int32)
    attended = lax.map(one_strip, starts).reshape(HEIGHT, WIDTH, D)
    block_out = (rolled_tok.astype(jnp.float32) + attended).astype(jnp.bfloat16)
    block_out = jnp.roll(block_out, (half, half), (0, 1))
    floats = block_out.astype(jnp.float32)
    pieces = []
    for scale_value in bin_scales:
        cell_mean = floats.reshape(scale_value, HEIGHT // scale_value, scale_value, WIDTH // scale_value, D).mean(axis=(1, 3))
        pieces.append(cell_mean.reshape(scale_value * scale_value, D))
    projected = branch_projections(jnp.concatenate(pieces, 0), branch_weight, branch_bias, join_branch)
    row_spread = bin_tables(jnp.arange(HEIGHT, dtype=jnp.int32), HEIGHT)[1]
    col_spread = bin_tables(jnp.arange(WIDTH, dtype=jnp.int32), WIDTH)[1]
    direct = jnp.dot(block_out.reshape(-1, D), join_block, preferred_element_type=jnp.float32).reshape(HEIGHT, WIDTH, CH)
    pre_norm = direct + spread_cells(projected, row_spread, col_spread)
    mean_val = lax.optimization_barrier(jnp.mean(pre_norm, axis=(0, 1)))
    variance = lax.optimization_barrier(jnp.mean(jnp.square(pre_norm - mean_val), axis=(0, 1)))
    joined = jax.nn.relu((pre_norm - mean_val) * lax.rsqrt(variance + norm_eps) * bn_gain + bn_bias)
    return joined.astype(jnp.bfloat16)
```

```python
import functools

import jax
import jax.numpy as jnp
import numpy as np
from jax import lax
from jax.experimental import pallas as pl
from jax.experimental.pallas import tpu as pltpu
from jax.sharding import PartitionSpec as P

WIN = 12
HALF = 6
HEADS = 24
D = 768
CH = 512
HEIGHT = 768
WIDTH = 96
ROWS = 12
COLS = 24
TOK = ROWS * COLS
NW = WIN * WIN
EPS = 1e-5
F32 = jnp.float32
BF16 = jnp.bfloat16
HIGHEST = lax.Precision.HIGHEST
MESH = pl.DeviceIdType.MESH
VMEM = pl.BlockSpec(memory_space=pltpu.VMEM)
ANY = pl.BlockSpec(memory_space=pl.ANY)


def dot(a, b):
    return jnp.dot(a, b, preferred_element_type=F32)


def dot_exact(a, b):
    return jnp.dot(a, b, preferred_element_type=F32, precision=HIGHEST)


def hats(count, total):
    place = np.arange(total) + 0.5
    source = np.clip(place * count / total - 0.5, 0, count - 1)
    return np.maximum(0, 1 - np.abs(source[:, None] - np.arange(count)[None, :]))


def make_tables():
    t = {}
    perm_in = np.zeros((TOK, 384), np.float32)
    perm_out = np.zeros((320, TOK), np.float32)
    perm_fin = np.zeros((TOK, 320), np.float32)
    place = np.zeros((8, TOK), np.float32)
    for w in range(2):
        for p in range(WIN):
            for q in range(WIN):
                row, jj = w * NW + p * WIN + q, w * WIN + q
                low, edge = p >= HALF, jj >= COLS - HALF
                pp = p - HALF if low else p
                if not edge:
                    src = (NW if low else 0) + pp * COLS + HALF + jj
                    dst = (112 if low else 0) + pp * 18 + jj
                else:
                    src = 288 + (48 if low else 0) + pp * 8 + jj - 18
                    dst = 224 + (48 if low else 0) + pp * 6 + jj - 18
                perm_in[row, src] = 1
                perm_out[dst, row] = 1
                i = pp if low else pp + HALF
                j = jj - 18 if edge else jj + HALF
                perm_fin[i * COLS + j, dst] = 1
                place[0, row], place[1, row] = p, jj
    t["perm_in"], t["perm_out"], t["perm_fin"] = perm_in, perm_out, perm_fin
    t["place"] = place
    spot = np.zeros((TOK, 8), np.float32)
    spot[:, 0] = np.arange(TOK) // COLS
    spot[:, 1] = np.arange(TOK) % COLS
    t["spot"] = spot
    cells = np.full((48, 8), -9.0, np.float32)
    cells[:, 2] = 6
    for k in range(36):
        cells[k, :3] = (k // 6, k % 6, 6)
    for k in range(9):
        cells[36 + k, :3] = (k // 3, k % 3, 3)
    t["cells"] = cells
    t["cells_t"] = np.ascontiguousarray(cells.T)
    gather = np.zeros((96, 40), np.float32)
    inverse = np.zeros((96, 1), np.float32)
    mix = np.zeros((48, 96), np.float64)
    half_hat = np.array([[1, 1, 2 / 3, 1 / 3, 0, 0], [0, 0, 1 / 3, 2 / 3, 1, 1]])
    for scale, base in ((6, 0), (3, 48), (2, 64), (1, 80)):
        for a in range(scale):
            for b in range(scale):
                at = base + a * scale + b
                step = 6 // scale
                for u in range(step):
                    for v in range(step):
                        gather[at, (a * step + u) * 6 + b * step + v] = 1
                inverse[at] = (scale / HEIGHT) * (scale / WIDTH)
                if scale == 6:
                    mix[a * 6 + b, at] = 1
                elif scale == 3:
                    mix[36 + a * 3 + b, at] = 1
                elif scale == 2:
                    for m in range(6):
                        for n in range(6):
                            mix[m * 6 + n, at] = half_hat[a, m] * half_hat[b, n]
                else:
                    mix[:36, at] = 1
    t["gather"], t["inverse"], t["mix"] = gather, inverse, mix
    r6, c6, r3, c3 = hats(6, HEIGHT), hats(6, WIDTH), hats(3, HEIGHT), hats(3, WIDTH)
    rr = np.zeros((HEIGHT, 48))
    cc = np.zeros((WIDTH, 48))
    for k in range(36):
        rr[:, k], cc[:, k] = r6[:, k // 6], c6[:, k % 6]
    for k in range(9):
        rr[:, 36 + k], cc[:, 36 + k] = r3[:, k // 3], c3[:, k % 3]
    t["gram"] = (rr.T @ rr) * (cc.T @ cc)
    t["mass"] = (rr.sum(0) * cc.sum(0))[:, None]
    bf = ("perm_in", "perm_out", "perm_fin")
    return {k: np.asarray(v, BF16 if k in bf else np.float32) for k, v in t.items()}


def halo_kernel(tok, down, right, diag, send, recv):
    r, c = lax.axis_index("rows"), lax.axis_index("cols")
    nr, nc = lax.axis_size("rows"), lax.axis_size("cols")
    r_next, c_next = lax.rem(r + 1, nr), lax.rem(c + 1, nc)
    r_prev, c_prev = lax.rem(r + nr - 1, nr), lax.rem(c + nc - 1, nc)
    barrier = pltpu.get_barrier_semaphore()
    for to in ((r_next, c), (r, c_next), (r_next, c_next)):
        pl.semaphore_signal(barrier, inc=1, device_id=to, device_id_type=MESH)
    pl.semaphore_wait(barrier, 3)
    copies = []
    plan = (
        (tok.at[pl.ds(0, HALF)], down, (r_prev, c)),
        (tok.at[pl.ds(HALF, HALF), pl.ds(0, 8)], right, (r, c_prev)),
        (tok.at[pl.ds(0, HALF), pl.ds(0, 8)], diag, (r_prev, c_prev)),
    )
    for n, (src, dst, to) in enumerate(plan):
        copy = pltpu.make_async_remote_copy(
            src_ref=src, dst_ref=dst, send_sem=send.at[n], recv_sem=recv.at[n],
            device_id=to, device_id_type=MESH,
        )
        copy.start()
        copies.append(copy)
    for copy in copies:
        copy.wait()


def token_halo(tokens):
    return pl.pallas_call(
        halo_kernel,
        out_shape=(
            jax.ShapeDtypeStruct((HALF, COLS, D), BF16),
            jax.ShapeDtypeStruct((HALF, 8, D), BF16),
            jax.ShapeDtypeStruct((HALF, 8, D), BF16),
        ),
        in_specs=[ANY],
        out_specs=(ANY, ANY, ANY),
        scratch_shapes=[pltpu.SemaphoreType.DMA((3,)), pltpu.SemaphoreType.DMA((3,))],
        compiler_params=pltpu.CompilerParams(collective_id=0, has_side_effects=True),
        name="halo",
    )(tokens)


def block_kernel(
    tok, down, right, diag, perm_in, ln_gain, ln_bias, wqkv, bqkv, tab0, tab1, wproj, bproj,
    join, perm_out, place, cells, pay, moved, bias, bias_tail, qkv, xw, ctx, mask,
):
    r, c = lax.axis_index("rows"), lax.axis_index("cols")
    lane = lax.broadcasted_iota(jnp.int32, (HEADS, 384), 1)
    col = lax.rem(lane, WIN)
    for q in range(WIN):
        d = WIN - 1 - q
        base = tab0[...]
        if d:
            base = jnp.where(
                col < WIN - d,
                pltpu.roll(base, 384 - d, 1),
                pltpu.roll(tab1[...], WIN - d, 1),
            )
        for p in range(WIN):
            shift = (WIN - 1 - p) * WIN
            at = (p * WIN + q) * HEADS
            bias[at : at + HEADS, :] = base[:, shift : shift + 128]
            bias_tail[at : at + HEADS, :] = base[:, shift + 16 : shift + NW]

    iq = lax.broadcasted_iota(jnp.int32, (NW, NW), 0)
    ik = lax.broadcasted_iota(jnp.int32, (NW, NW), 1)
    row_cut = (iq >= NW // 2) != (ik >= NW // 2)
    col_cut = (lax.rem(iq, WIN) >= HALF) != (lax.rem(ik, WIN) >= HALF)
    last_row = jnp.where(r == lax.axis_size("rows") - 1, -100.0, 0.0).astype(F32)
    last_col = jnp.where(c == lax.axis_size("cols") - 1, -100.0, 0.0).astype(F32)
    by_row = jnp.where(row_cut, last_row, 0.0)
    mask[0] = by_row
    mask[1] = jnp.minimum(by_row, jnp.where(col_cut, last_col, 0.0))

    raw = jnp.concatenate([tok[NW : 2 * NW, :], down[...], right[...], diag[...]], 0)
    x = dot(perm_in[...], raw)
    xw[...] = x
    center = jnp.mean(x, -1, keepdims=True)
    cent = x - center
    spread = jnp.mean(cent * cent, -1, keepdims=True)
    normed = (cent * lax.rsqrt(spread + EPS) * ln_gain[...] + ln_bias[...]).astype(BF16)

    for n in range(9):
        part = slice(n * 256, (n + 1) * 256)
        acc = dot(normed, wqkv[:, part]) + bqkv[:, part]
        if n < 3:
            acc = acc * (32**-0.5)
        qkv[:, part] = acc.astype(BF16)

    lane_head = lax.broadcasted_iota(jnp.int32, (NW, 128), 1) // 32

    def group(g, carry):
        at = pl.multiple_of(g * 128, 128)
        for w in range(2):
            rows = pl.ds(w * NW, NW)
            qg = qkv[rows, pl.ds(at, 128)]
            kg = qkv[rows, pl.ds(pl.multiple_of(at + D, 128), 128)]
            vg = qkv[rows, pl.ds(pl.multiple_of(at + 2 * D, 128), 128)]
            out = jnp.zeros((NW, 128), F32)
            for h in range(4):
                qm = jnp.where(lane_head == h, qg, jnp.zeros_like(qg))
                s = lax.dot_general(qm, kg, (((1,), (1,)), ((), ())), preferred_element_type=F32)
                pick = pl.ds(g * 4 + h, NW, stride=HEADS)
                pair = jnp.concatenate([bias[pick, :], bias_tail[pick, :][:, 112:]], 1)
                s = s + pair + mask[w]
                e = jnp.exp(s - jnp.max(s, -1, keepdims=True))
                total = jnp.sum(e, -1, keepdims=True)
                o = dot(e.astype(BF16), vg) * (1.0 / total)
                out = jnp.where(lane_head == h, o, out)
            ctx[rows, pl.ds(at, 128)] = out.astype(BF16)
        return carry

    lax.fori_loop(0, 6, group, 0)

    block = (xw[...] + (dot(ctx[...], wproj[...]) + bproj[...])).astype(BF16)
    direct = dot(block, join[...])
    squares = jnp.sum(direct * direct, 0, keepdims=True)

    irow = place[0:1, :] + (r * ROWS + HALF).astype(F32)
    irow = jnp.where(irow >= HEIGHT, irow - HEIGHT, irow)
    icol = place[1:2, :] + (c * COLS + HALF).astype(F32)
    icol = jnp.where(icol >= WIDTH, icol - WIDTH, icol)
    ca, cb, cs = cells[:, 0:1], cells[:, 1:2], cells[:, 2:3]
    inside = (
        (irow >= ca[:40] * 128.0) & (irow < ca[:40] * 128.0 + 128.0)
        & (icol >= cb[:40] * 16.0) & (icol < cb[:40] * 16.0 + 16.0)
        & (cs[:40] > 4.0)
    )
    pooled = dot(jnp.where(inside, 1.0, 0.0).astype(BF16), block)
    row_at = jnp.clip((irow + 0.5) * (cs * (1.0 / HEIGHT)) - 0.5, 0.0, cs - 1.0)
    col_at = jnp.clip((icol + 0.5) * (cs * (1.0 / WIDTH)) - 0.5, 0.0, cs - 1.0)
    hat = jnp.maximum(1.0 - jnp.abs(row_at - ca), 0.0) * jnp.maximum(1.0 - jnp.abs(col_at - cb), 0.0)
    weighted = dot_exact(hat, direct)
    row_id = lax.broadcasted_iota(jnp.int32, (48, 1), 0)
    weighted = jnp.where(row_id == 45, squares, weighted)
    for n in range(6):
        pay[n * 40 : n * 40 + 40, :] = pooled[:, n * 128 : (n + 1) * 128]
    for n in range(4):
        pay[240 + n * 48 : 288 + n * 48, :] = weighted[:, n * 128 : (n + 1) * 128]
    pay[432:, :] = jnp.zeros((80, 128), F32)
    moved[...] = dot(perm_out[...], block).astype(BF16)


def reduce_kernel(pay, moved, full, halo, rs, zs, rs_send, rs_recv, z_send, z_recv, g_send, g_recv, h_send, h_recv):
    r, c = lax.axis_index("rows"), lax.axis_index("cols")
    nr, nc = lax.axis_size("rows"), lax.axis_size("cols")
    z = lax.rem(r // 4, 8)
    me = (r // 32) * 16 + lax.rem(r, 4) * 4 + c
    r_next, c_next = lax.rem(r + 1, nr), lax.rem(c + 1, nc)
    r_prev, c_prev = lax.rem(r + nr - 1, nr), lax.rem(c + nc - 1, nc)

    def plane(step):
        j = lax.rem(me + step, 32)
        return j, ((j // 16) * 32 + z * 4 + lax.rem(j // 4, 4), lax.rem(j, 4))

    def column(step):
        k = lax.rem(z + step, 8)
        return k, ((r // 32) * 32 + k * 4 + lax.rem(r, 4), c)

    barrier = pltpu.get_barrier_semaphore()

    def greet_plane(step, carry):
        _, to = plane(step)
        pl.semaphore_signal(barrier, inc=1, device_id=to, device_id_type=MESH)
        return carry

    def greet_column(step, carry):
        _, to = column(step)
        pl.semaphore_signal(barrier, inc=1, device_id=to, device_id_type=MESH)
        return carry

    lax.fori_loop(1, 8, greet_column, 0)
    lax.fori_loop(1, 32, greet_plane, 0)
    for to in ((r_prev, c), (r, c_prev), (r_prev, c_prev)):
        pl.semaphore_signal(barrier, inc=1, device_id=to, device_id_type=MESH)
    pl.semaphore_wait(barrier, 41)

    def remote(src, dst, s, v, to):
        return pltpu.make_async_remote_copy(
            src_ref=src, dst_ref=dst, send_sem=s, recv_sem=v, device_id=to, device_id_type=MESH
        )

    def rs_start(step, carry):
        j, to = plane(step)
        remote(pay.at[j], rs.at[me], rs_send, rs_recv, to).start()
        return carry

    lax.fori_loop(1, 32, rs_start, 0)
    halos = []
    for n, (src, dst, to) in enumerate(
        (
            (moved.at[pl.ds(112, 112)], halo.at[pl.ds(0, 112)], (r_next, c)),
            (moved.at[pl.ds(224, 48)], halo.at[pl.ds(112, 48)], (r, c_next)),
            (moved.at[pl.ds(272, 48)], halo.at[pl.ds(160, 48)], (r_next, c_next)),
        )
    ):
        copy = remote(src, dst, h_send.at[n], h_recv.at[n], to)
        copy.start()
        halos.append(copy)

    rs[me] = pay[me]
    remote(rs.at[pl.ds(0, 31)], rs.at[pl.ds(0, 31)], rs_send, rs_recv, (r_next, c)).wait_recv()
    zs[z] = jnp.sum(rs[...], 0)

    def z_start(step, carry):
        _, to = column(step)
        remote(zs.at[z], zs.at[z], z_send, z_recv, to).start()
        return carry

    lax.fori_loop(1, 8, z_start, 0)
    remote(zs.at[pl.ds(0, 7)], zs.at[pl.ds(0, 7)], z_send, z_recv, (r_next, c)).wait_recv()
    full[me] = jnp.sum(zs[...], 0)

    def g_start(step, carry):
        _, to = plane(step)
        remote(full.at[me], full.at[me], g_send, g_recv, to).start()
        return carry

    lax.fori_loop(1, 32, g_start, 0)
    remote(full.at[pl.ds(0, 31)], full.at[pl.ds(0, 31)], g_send, g_recv, (r_next, c)).wait_recv()
    for copy in halos:
        copy.wait()
    remote(rs.at[pl.ds(0, 31)], rs.at[pl.ds(0, 31)], rs_send, rs_recv, (r_next, c)).wait_send()
    remote(zs.at[pl.ds(0, 7)], zs.at[pl.ds(0, 7)], z_send, z_recv, (r_next, c)).wait_send()
    remote(full.at[pl.ds(0, 31)], full.at[pl.ds(0, 31)], g_send, g_recv, (r_next, c)).wait_send()


def reduce_all(pay, moved):
    dma = pltpu.SemaphoreType.DMA
    return pl.pallas_call(
        reduce_kernel,
        out_shape=(
            jax.ShapeDtypeStruct((32, 16, 128), F32),
            jax.ShapeDtypeStruct((208, D), BF16),
        ),
        in_specs=[VMEM, VMEM],
        out_specs=(VMEM, VMEM),
        scratch_shapes=[
            pltpu.VMEM((32, 16, 128), F32), pltpu.VMEM((8, 16, 128), F32),
            dma, dma, dma, dma, dma, dma, dma((3,)), dma((3,)),
        ],
        compiler_params=pltpu.CompilerParams(collective_id=1, has_side_effects=True),
        name="reduce",
    )(pay, moved)


def twice(values, weight):
    high = values.astype(BF16)
    low = (values - high.astype(F32)).astype(BF16)
    rows = values.shape[0]
    both = dot(jnp.concatenate([high, low], 0), weight)
    return both[:rows] + both[rows:]


def head_kernel(
    full, moved, halo, perm_fin, join, wbranch, bbranch, wjoin, bn_gain, bn_bias, gather, inverse,
    mix, gram, mass, spot, cells_t, out,
):
    r, c = lax.axis_index("rows"), lax.axis_index("cols")
    pooled = jnp.concatenate([full[n * 40 : n * 40 + 40, :] for n in range(6)], 1)
    weighted = jnp.concatenate([full[240 + n * 48 : 288 + n * 48, :] for n in range(4)], 1)
    means = dot_exact(gather[...], pooled) * inverse[...]
    parts = []
    for k, start, stop in ((3, 0, 48), (2, 48, 64), (1, 64, 80), (0, 80, 96)):
        hidden = twice(means[start:stop], wbranch[k]) + bbranch[k : k + 1, :]
        parts.append(twice(jnp.maximum(hidden, 0.0), wjoin[k]))
    lift = dot_exact(mix[...], jnp.concatenate(parts, 0))
    everyone = float(HEIGHT * WIDTH)
    total = jnp.sum(weighted[:36], 0, keepdims=True) + jnp.sum(mass[...] * lift, 0, keepdims=True)
    squares = (
        weighted[45:46]
        + 2.0 * jnp.sum(lift * weighted, 0, keepdims=True)
        + jnp.sum(lift * dot_exact(gram[...], lift), 0, keepdims=True)
    )
    mean_val = total * (1.0 / everyone)
    variance = squares * (1.0 / everyone) - mean_val * mean_val
    scale = bn_gain[...] * lax.rsqrt(variance + EPS)
    shift = bn_bias[...] - mean_val * scale
    x = dot(perm_fin[...], jnp.concatenate([moved[0:112, :], halo[...]], 0)).astype(BF16)
    direct = dot(x, join[...])
    irow = spot[:, 0:1] + (r * ROWS).astype(F32)
    icol = spot[:, 1:2] + (c * COLS).astype(F32)
    ca, cb, cs = cells_t[0:1, :], cells_t[1:2, :], cells_t[2:3, :]
    row_at = jnp.clip((irow + 0.5) * (cs * (1.0 / HEIGHT)) - 0.5, 0.0, cs - 1.0)
    col_at = jnp.clip((icol + 0.5) * (cs * (1.0 / WIDTH)) - 0.5, 0.0, cs - 1.0)
    hat = jnp.maximum(1.0 - jnp.abs(row_at - ca), 0.0) * jnp.maximum(1.0 - jnp.abs(col_at - cb), 0.0)
    pre = direct + dot_exact(hat, lift)
    out[...] = jnp.maximum(pre * scale + shift, 0.0).astype(BF16)


def shards(
    tokens, ln_gain, ln_bias, qkv_weight, qkv_bias, rel_table, proj_weight, proj_bias,
    branch_weight, branch_bias, join_block, join_branch, bn_gain, bn_bias,
):
    t = make_tables()
    down, right, diag = token_halo(tokens)
    table = rel_table[::-1, ::-1].transpose(2, 0, 1)
    tab0 = jnp.pad(table[:, :, :WIN].reshape(HEADS, 276), ((0, 0), (0, 108)))
    tab1 = jnp.pad(table[:, :, WIN:], ((0, 0), (0, 0), (0, 1))).reshape(HEADS, 276)
    tab1 = jnp.pad(tab1, ((0, 0), (0, 108)))
    pay, moved = pl.pallas_call(
        block_kernel,
        out_shape=(
            jax.ShapeDtypeStruct((512, 128), F32),
            jax.ShapeDtypeStruct((320, D), BF16),
        ),
        in_specs=[VMEM] * 17,
        out_specs=(VMEM, VMEM),
        scratch_shapes=[
            pltpu.VMEM((NW * HEADS, 128), F32),
            pltpu.VMEM((NW * HEADS, 128), F32),
            pltpu.VMEM((TOK, 3 * D), BF16),
            pltpu.VMEM((TOK, D), F32),
            pltpu.VMEM((TOK, D), BF16),
            pltpu.VMEM((2, NW, NW), F32),
        ],
        compiler_params=pltpu.CompilerParams(vmem_limit_bytes=40 * 2**20),
        name="block",
    )(
        tokens.reshape(TOK, D), down.reshape(NW, D), right.reshape(48, D), diag.reshape(48, D),
        t["perm_in"], ln_gain[None], ln_bias[None], qkv_weight, qkv_bias[None], tab0, tab1,
        proj_weight, proj_bias[None], join_block, t["perm_out"], t["place"], t["cells"],
    )
    full, halo = reduce_all(pay.reshape(32, 16, 128), moved)
    out = pl.pallas_call(
        head_kernel,
        out_shape=jax.ShapeDtypeStruct((TOK, CH), BF16),
        in_specs=[VMEM] * 17,
        out_specs=VMEM,
        compiler_params=pltpu.CompilerParams(vmem_limit_bytes=40 * 2**20),
        name="head",
    )(
        full.reshape(512, 128), moved, halo, t["perm_fin"], join_block, branch_weight, branch_bias,
        join_branch, bn_gain[None], bn_bias[None], t["gather"], t["inverse"], t["mix"], t["gram"],
        t["mass"], t["spot"], t["cells_t"],
    )
    return out.reshape(ROWS, COLS, CH)


def solution(mesh):
    in_specs = (P("rows", "cols", None),) + (P(),) * 13
    return jax.shard_map(
        shards, mesh=mesh, in_specs=in_specs, out_specs=P("rows", "cols", None), check_vma=False
    )
```
